256 devices in a mesh: row: 32 (over y, x, core), col: 8 (over z).
Axes of the slice: x: 4, y: 4, z: 8, core: 2. Of those that a mesh axis runs over, the one named last changes fastest.
Arguments:
- vectors: float32 [16384, 16384], P('row', 'col'), may hold values from -0.046875 to 0.046875
- basis: float32 [16384, 2048], P('col', 'row'), may hold values from -9 to 9
- block_units: int32 [8], replicated, may hold values from 1 to 40, 64 in all
Outputs:
- assembled: float32 [16384, 2048], P('row', 'col')
The draws below stay inside these ranges and needn't reach their ends.
Inputs may be any that keep to these rules, and one draw needn't show every extreme that they name: `block_units`: the block sizes are whole numbers of units that sum to 64; the largest is exactly the maximum.
All inputs are finite; a program needn't handle non-finite values.
Results may differ from the reference program's by a relative error of at most 0.00007.
Values sent between devices are 32-bit elements; how exact they have to be, the bound alone decides.
A program may use at most 64 MiB of HBM per device.

```python
import math
import jax
import jax.numpy as jnp
import numpy as np
from jax import lax

N = 16384
W = 2048
UNIT = 256
BLOCKS = 8
START = 7168


def block_scale(own_key, extent, cuts, smallest, largest):
    def one(axis_at, shards_of):
        heights = jax.random.uniform(jax.random.fold_in(jax.random.fold_in(own_key, 6), axis_at), (shards_of,), jnp.float32, smallest / len(cuts), largest / len(cuts))
        return jnp.repeat(jnp.exp(heights), extent[axis_at] // shards_of).reshape((-1,) + (1,) * (len(extent) - axis_at - 1))

    level = one(*cuts[0])
    for cut in cuts[1:]:
        level = level * one(*cut)
    return level


def length_profile(count, total, reach, skew):
    weights = [(1 << 20) // math.isqrt(standing ** skew) + 1 for standing in range(2, count + 1)]
    surplus, counts = total - reach - (count - 1), [1] * (count - 1)
    while surplus > 0:
        candidates = [i for i in range(count - 1) if counts[i] < reach]
        mass, left = sum([weights[i] for i in candidates]), surplus
        for i in candidates:
            extra = min(reach - counts[i], max(1, left * weights[i] // mass), surplus)
            counts[i] = counts[i] + extra
            surplus = surplus - extra
    return np.array([reach] + counts)


def uneven_parts(key, amount, total, most, slope):
    if amount == 2:
        one = jax.random.randint(key, (), max(1, total - most), min(most, total - 1) + 1)
        return jnp.stack([one, total - one])
    tallies = jnp.asarray(length_profile(amount, total, most, slope), jnp.int32)
    couples = (amount - 1) // 2
    donor, receiver = tallies[1:1 + 2 * couples:2], tallies[2:2 + 2 * couples:2]
    room = jnp.minimum(donor - 1, most - receiver)
    moved = jax.random.randint(jax.random.fold_in(key, 1), (couples,), 0, 1 << 20) % (room + 1)
    tallies = tallies.at[1:1 + 2 * couples:2].set(donor - moved).at[2:2 + 2 * couples:2].set(receiver + moved)
    return tallies[jax.random.permutation(jax.random.fold_in(key, 2), amount)]


def bell_draw(own_key, dims, spread, bound, pieces=(), held_as=jnp.bfloat16):
    array = spread * jax.random.normal(own_key, dims, jnp.float32)
    if pieces:
        array = array * block_scale(own_key, dims, pieces, -0.22, 0.18)
    return jnp.clip(array, -bound, bound).astype(held_as)


def setup_inputs(seed: int = 0) -> dict:
    key_list = jax.random.split(jax.random.key(seed), 4)
    return {
        "vectors": bell_draw(key_list[0], (N, N), N ** -0.5, 0.046875, ((0, 32), (1, 8)), jnp.float32),
        "basis": bell_draw(key_list[1], (N, W), 1.5, 9.0, ((0, 8), (1, 32)), jnp.float32),
        "block_units": uneven_parts(key_list[2], BLOCKS, N // UNIT, 5 * N // (8 * UNIT), 2).astype(jnp.int32),
    }


def block_ids(positions, block_units):
    ends = jnp.cumsum(block_units).astype(jnp.int32) * UNIT
    return jnp.sum((positions[:, None] >= ends[None, :-1]).astype(jnp.int32), axis=1)


def reference(vectors, basis, block_units):
    row_block = block_ids(jnp.arange(N, dtype=jnp.int32), block_units)
    slab_block = block_ids(START + jnp.arange(W, dtype=jnp.int32), block_units)
    masked = jnp.where(row_block[:, None] == slab_block[None, :], basis, jnp.float32(0.0))
    return jnp.dot(vectors, masked, precision=lax.Precision.HIGHEST, preferred_element_type=jnp.float32)
```

```python
import functools

import jax
import jax.numpy as jnp
from jax import lax
from jax.experimental import pallas as pl
from jax.experimental.pallas import tpu as pltpu
from jax.sharding import PartitionSpec as P

MESH = pl.DeviceIdType.MESH
UNIT = 256
START = 7168
RINGS = 4
PHASES = 8


def kernel(dims, units_ref, v_hbm, bt_hbm, o_ref, gathered, v_mem, weights, lhs, part, up_first, up_rest, down_first,
           down_rest, local_sem, own_sem, gather_sem, gather_sent, mate_sem, mate_sent, sum_sem, sum_sent):
    rows, depth, own, devices, planes = dims
    step = own // PHASES
    width = step * devices
    half = depth // 2
    chunk = width // planes
    per_keep = own * devices // planes // own

    me = lax.axis_index("row")
    z = lax.axis_index("col")
    core = lax.rem(me, 2)
    x = lax.rem(lax.div(me, 2), RINGS)
    y = lax.div(me, 2 * RINGS)

    def at(xx, yy):
        return (yy * RINGS + xx) * 2 + core

    def shift(c, by, n):
        return lax.rem(c + (by % n), n)

    mate = me + 1 - 2 * core
    neighbour = {
        ("x", 1): (at(shift(x, 1, RINGS), y), z),
        ("x", -1): (at(shift(x, -1, RINGS), y), z),
        ("y", 1): (at(x, shift(y, 1, RINGS)), z),
        ("y", -1): (at(x, shift(y, -1, RINGS)), z),
    }
    mate_id = (mate, z)
    up_id = (me, shift(z, 1, planes))
    down_id = (me, shift(z, -1, planes))
    axes = (("x", "y"), ("y", "x"))

    load_v = pltpu.make_async_copy(v_hbm, v_mem, local_sem)
    load_v.start()
    for q in range(PHASES):
        pltpu.make_async_copy(
            bt_hbm.at[pl.ds(q * step, step)],
            gathered.at[q, pl.ds(pl.multiple_of(me * step, step), step)],
            own_sem.at[q],
        ).start()

    barrier = pltpu.get_barrier_semaphore()
    for other in (*neighbour.values(), mate_id, up_id, down_id):
        pl.semaphore_signal(barrier, inc=1, device_id=other, device_id_type=MESH)
    pl.semaphore_wait(barrier, 7)

    def piece(q, h, fo, so):
        if h == 0:
            source = at(shift(x, fo, RINGS), shift(y, so, RINGS))
        else:
            source = at(shift(x, so, RINGS), shift(y, fo, RINGS))
        return gathered.at[q, pl.ds(pl.multiple_of(source * step, step), step), pl.ds(h * half, half)]

    def send(q, h, fo, so, which, direction):
        ref = piece(q, h, fo, so)
        nfo, nso = (fo - direction, so) if which == 0 else (fo, so - direction)
        pltpu.make_async_remote_copy(
            src_ref=ref,
            dst_ref=ref,
            send_sem=gather_sent.at[q],
            recv_sem=gather_sem.at[q, h, (nfo % RINGS) * RINGS + nso % RINGS],
            device_id=neighbour[axes[h][which], direction],
            device_id_type=MESH,
        ).start()

    def arrived(q, h, fo, so):
        ref = piece(q, h, fo, so)
        pltpu.make_async_copy(ref, ref, gather_sem.at[q, h, (fo % RINGS) * RINGS + so % RINGS]).wait()

    def share(q, h, fo, so):
        ref = piece(q, h, fo, so)
        pltpu.make_async_remote_copy(
            src_ref=ref, dst_ref=ref, send_sem=mate_sent.at[q], recv_sem=mate_sem.at[q], device_id=mate_id, device_id_type=MESH
        ).start()

    def first_way(q, h):
        return 1 if (q + h) % 2 == 0 else -1

    def second_way(q, h, fo):
        return 1 if (q + fo // 2 + fo) % 2 == 0 else -1

    def level0(q):
        pltpu.make_async_copy(
            bt_hbm.at[pl.ds(q * step, step)],
            gathered.at[q, pl.ds(pl.multiple_of(me * step, step), step)],
            own_sem.at[q],
        ).wait()
        for h in range(2):
            for direction in (1, -1):
                send(q, h, 0, 0, 0, direction)
        for h in range(2):
            for direction in (1, -1):
                send(q, h, 0, 0, 1, direction)
        for h in range(2):
            share(q, h, 0, 0)

    def along_second(q, h, fo):
        for direction in (1, -1):
            send(q, h, fo, 0, 1, direction)
        share(q, h, fo, 0)

    def level1(q):
        for fo in (-1, 1):
            for h in range(2):
                arrived(q, h, fo, 0)
                if first_way(q, h) == -fo:
                    send(q, h, fo, 0, 0, -fo)
                along_second(q, h, fo)

    def cross(q, h, fo):
        for so in (-1, 1):
            arrived(q, h, fo, so)
            if second_way(q, h, fo) == -so:
                send(q, h, fo, so, 1, -so)
            share(q, h, fo, so)

    def level2(q):
        for h in range(2):
            cross(q, h, 0)
        for h in range(2):
            arrived(q, h, 2, 0)
            along_second(q, h, 2)

    def level3(q):
        for fo in (-1, 1, 2):
            for h in range(2):
                cross(q, h, fo)

    def level4(q):
        for fo in (0, -1, 1, 2):
            for h in range(2):
                arrived(q, h, fo, 2)
                share(q, h, fo, 2)

    def prepare():
        load_v.wait()
        tile = 256

        def body(t, _):
            at_k = pl.multiple_of(t * tile, tile)
            block = v_mem[:, pl.ds(at_k, tile)].T
            hi = block.astype(jnp.bfloat16)
            lo = (block - hi.astype(jnp.float32)).astype(jnp.bfloat16)
            weights[pl.ds(at_k, tile), :] = hi
            weights[pl.ds(pl.multiple_of(depth + at_k, tile), tile), :] = lo
            weights[pl.ds(pl.multiple_of(2 * depth + at_k, tile), tile), :] = hi
            return 0

        lax.fori_loop(0, depth // tile, body, 0)

    ends = []
    total = 0
    for b in range(7):
        total = total + units_ref[b] * UNIT
        ends.append(total)

    def block_of(position):
        ids = jnp.zeros_like(position)
        for end in ends:
            ids = ids + (position >= end).astype(jnp.int32)
        return ids

    def multiply(q):
        group = 16
        row_block = block_of(z * depth + lax.broadcasted_iota(jnp.int32, (1, depth), 1))

        def split(g, _):
            first = pl.multiple_of(g * group, group)
            index = first + lax.broadcasted_iota(jnp.int32, (group, 1), 0)
            column = lax.div(index, step) * own + q * step + lax.rem(index, step)
            keep = block_of(START + column) == row_block
            block = jnp.where(keep, gathered[q, pl.ds(first, group), :], 0.0)
            hi = block.astype(jnp.bfloat16)
            lo = (block - hi.astype(jnp.float32)).astype(jnp.bfloat16)
            lhs[pl.ds(first, group), 0:depth] = hi
            lhs[pl.ds(first, group), depth:2 * depth] = hi
            lhs[pl.ds(first, group), 2 * depth:3 * depth] = lo
            return 0

        lax.fori_loop(0, width // group, split, 0)
        part[q] = jnp.dot(lhs[...], weights[...], preferred_element_type=jnp.float32)

    def chunk_rows(plane, start=0, size=chunk):
        return pl.ds(pl.multiple_of(plane * chunk + start, 8), size)

    def sum_copy(q, s, direction):
        if s == 1:
            start = 0 if direction == 1 else chunk // 2
            src = part.at[q, chunk_rows(shift(z, 4, planes), start, chunk // 2)]
            dst = (up_first if direction == 1 else down_first).at[q]
        else:
            src = part.at[q, chunk_rows(shift(z, direction * (5 - s), planes))]
            dst = (up_rest if direction == 1 else down_rest).at[q, s - 2]
        lane = 0 if direction == 1 else 1
        return pltpu.make_async_remote_copy(
            src_ref=src,
            dst_ref=dst,
            send_sem=sum_sent.at[q, lane, s - 1],
            recv_sem=sum_sem.at[q, lane, s - 1],
            device_id=up_id if direction == 1 else down_id,
            device_id_type=MESH,
        )

    def sum_first(q):
        for direction in (1, -1):
            sum_copy(q, 1, direction).start()

    def sum_next(q, s):
        for direction in (1, -1):
            sum_copy(q, s - 1, direction).wait_recv()
            got = up_first if direction == 1 else down_first
            target = shift(z, direction * (5 - s), planes)
            if s == 2:
                start = 0 if direction == 1 else chunk // 2
                where = chunk_rows(target, start, chunk // 2)
                part[q, where, :] = part[q, where, :] + got[q]
            else:
                got = up_rest if direction == 1 else down_rest
                where = chunk_rows(target)
                part[q, where, :] = part[q, where, :] + got[q, s - 3]
            sum_copy(q, s, direction).start()

    def sum_last(q):
        for direction in (1, -1):
            sum_copy(q, 4, direction).wait_recv()
        total = part[q, chunk_rows(z), :] + up_rest[q, 2] + down_rest[q, 2]
        for i in range(per_keep):
            o_ref[i * own + q * step:i * own + (q + 1) * step, :] = total[i * step:(i + 1) * step, :]

    def sums(q, s):
        if 0 <= q < PHASES:
            if s == 1:
                sum_first(q)
            elif s == 5:
                sum_last(q)
            else:
                sum_next(q, s)

    def drain(q):
        n = 2 * (RINGS * RINGS - 1)
        ref = gathered.at[q, pl.ds(0, n // 2 * step)]
        pltpu.make_async_copy(ref, ref, gather_sent.at[q]).wait()
        ref = gathered.at[q, pl.ds(0, RINGS * RINGS * step)]
        pltpu.make_async_copy(ref, ref, mate_sent.at[q]).wait()
        for s in range(1, 5):
            for direction in (1, -1):
                sum_copy(q, s, direction).wait_send()

    def mate_arrived(q):
        ref = gathered.at[q, pl.ds(0, RINGS * RINGS * step)]
        pltpu.make_async_copy(ref, ref, mate_sem.at[q]).wait()

    level0(0)
    level0(1)
    prepare()
    level1(0)
    for q in range(PHASES):
        level2(q)
        level3(q)
        sums(q - 1, 2)
        sums(q - 2, 4)
        if q + 2 < PHASES:
            level0(q + 2)
        if q + 1 < PHASES:
            level1(q + 1)
        level4(q)
        sums(q - 1, 3)
        sums(q - 2, 5)
        mate_arrived(q)
        multiply(q)
        sums(q, 1)
    sums(PHASES - 2, 4)
    sums(PHASES - 1, 2)
    sums(PHASES - 2, 5)
    sums(PHASES - 1, 3)
    sums(PHASES - 1, 4)
    for q in range(PHASES):
        drain(q)
    sums(PHASES - 1, 5)


def solution(mesh):
    devices, planes = mesh.shape["row"], mesh.shape["col"]

    def body(vectors, basis, block_units):
        rows, depth = vectors.shape
        own = basis.shape[1]
        step = own // PHASES
        width = step * devices
        chunk = width // planes
        f32, bf16 = jnp.float32, jnp.bfloat16
        summed = pl.pallas_call(
            functools.partial(kernel, (rows, depth, own, devices, planes)),
            out_shape=jax.ShapeDtypeStruct((own * devices // planes, rows), f32),
            in_specs=[
                pl.BlockSpec(memory_space=pltpu.SMEM),
                pl.BlockSpec(memory_space=pl.ANY),
                pl.BlockSpec(memory_space=pl.ANY),
            ],
            out_specs=pl.BlockSpec(memory_space=pltpu.VMEM),
            scratch_shapes=[
                pltpu.VMEM((PHASES, width, depth), f32),
                pltpu.VMEM((rows, depth), f32),
                pltpu.VMEM((3 * depth, rows), bf16),
                pltpu.VMEM((width, 3 * depth), bf16),
                pltpu.VMEM((PHASES, width, rows), f32),
                pltpu.VMEM((PHASES, chunk // 2, rows), f32),
                pltpu.VMEM((PHASES, 3, chunk, rows), f32),
                pltpu.VMEM((PHASES, chunk // 2, rows), f32),
                pltpu.VMEM((PHASES, 3, chunk, rows), f32),
                pltpu.SemaphoreType.DMA,
                pltpu.SemaphoreType.DMA((PHASES,)),
                pltpu.SemaphoreType.DMA((PHASES, 2, RINGS * RINGS)),
                pltpu.SemaphoreType.DMA((PHASES,)),
                pltpu.SemaphoreType.DMA((PHASES,)),
                pltpu.SemaphoreType.DMA((PHASES,)),
                pltpu.SemaphoreType.DMA((PHASES, 2, 4)),
                pltpu.SemaphoreType.DMA((PHASES, 2, 4)),
            ],
            compiler_params=pltpu.CompilerParams(
                collective_id=0, has_side_effects=True, vmem_limit_bytes=63 * 1024 * 1024
            ),
            cost_estimate=pl.CostEstimate(
                flops=6 * rows * depth * own * devices, bytes_accessed=4 * rows * depth, transcendentals=0
            ),
        )(block_units, vectors, basis.T)
        return summed.T

    return jax.shard_map(
        body,
        mesh=mesh,
        in_specs=(P("row", "col"), P("col", "row"), P()),
        out_specs=P("row", "col"),
        check_vma=False,
    )
```

```python
import functools

import jax
import jax.numpy as jnp
from jax import lax
from jax.experimental import pallas as pl
from jax.experimental.pallas import tpu as pltpu
from jax.sharding import PartitionSpec as P

MESH = pl.DeviceIdType.MESH
UNIT = 256
START = 7168
RINGS = 4
PHASES = 8
AHEAD = 2
LAG = 0
HOP_ORDER = (1, 2, 3, 4)


def kernel(dims, units_ref, v_hbm, bt_hbm, o_ref, gathered, v_mem, weights, lhs, part, up_first, up_rest, down_first,
           down_rest, local_sem, own_sem, gather_sem, gather_sent, mate_sem, mate_sent, sum_sem, sum_sent):
    rows, depth, own, devices, planes = dims
    step = own // PHASES
    width = step * devices
    half = depth // 2
    chunk = width // planes
    per_keep = own * devices // planes // own

    me = lax.axis_index("row")
    z = lax.axis_index("col")
    core = lax.rem(me, 2)
    x = lax.rem(lax.div(me, 2), RINGS)
    y = lax.div(me, 2 * RINGS)

    def at(xx, yy):
        return (yy * RINGS + xx) * 2 + core

    def shift(c, by, n):
        return lax.rem(c + (by % n), n)

    mate = me + 1 - 2 * core
    neighbour = {
        ("x", 1): (at(shift(x, 1, RINGS), y), z),
        ("x", -1): (at(shift(x, -1, RINGS), y), z),
        ("y", 1): (at(x, shift(y, 1, RINGS)), z),
        ("y", -1): (at(x, shift(y, -1, RINGS)), z),
    }
    mate_id = (mate, z)
    up_id = (me, shift(z, 1, planes))
    down_id = (me, shift(z, -1, planes))
    axes = (("x", "y"), ("y", "x"))

    load_v = pltpu.make_async_copy(v_hbm, v_mem, local_sem)
    load_v.start()
    for q in range(PHASES):
        pltpu.make_async_copy(
            bt_hbm.at[pl.ds(q * step, step)],
            gathered.at[q, pl.ds(pl.multiple_of(me * step, step), step)],
            own_sem.at[q],
        ).start()

    barrier = pltpu.get_barrier_semaphore()
    for other in (*neighbour.values(), mate_id, up_id, down_id):
        pl.semaphore_signal(barrier, inc=1, device_id=other, device_id_type=MESH)
    pl.semaphore_wait(barrier, 7)

    def piece(q, h, fo, so):
        if h == 0:
            source = at(shift(x, fo, RINGS), shift(y, so, RINGS))
        else:
            source = at(shift(x, so, RINGS), shift(y, fo, RINGS))
        return gathered.at[q, pl.ds(pl.multiple_of(source * step, step), step), pl.ds(h * half, half)]

    def send(q, h, fo, so, which, direction):
        ref = piece(q, h, fo, so)
        nfo, nso = (fo - direction, so) if which == 0 else (fo, so - direction)
        pltpu.make_async_remote_copy(
            src_ref=ref,
            dst_ref=ref,
            send_sem=gather_sent.at[q],
            recv_sem=gather_sem.at[q, h, (nfo % RINGS) * RINGS + nso % RINGS],
            device_id=neighbour[axes[h][which], direction],
            device_id_type=MESH,
        ).start()

    def arrived(q, h, fo, so):
        ref = piece(q, h, fo, so)
        pltpu.make_async_copy(ref, ref, gather_sem.at[q, h, (fo % RINGS) * RINGS + so % RINGS]).wait()

    def share(q, h, fo, so):
        ref = piece(q, h, fo, so)
        pltpu.make_async_remote_copy(
            src_ref=ref, dst_ref=ref, send_sem=mate_sent.at[q], recv_sem=mate_sem.at[q], device_id=mate_id, device_id_type=MESH
        ).start()

    def first_way(q, h):
        return 1 if (q + h) % 2 == 0 else -1

    def second_way(q, h, fo):
        return 1 if (q + fo // 2 + fo) % 2 == 0 else -1

    def level0(q):
        pltpu.make_async_copy(
            bt_hbm.at[pl.ds(q * step, step)],
            gathered.at[q, pl.ds(pl.multiple_of(me * step, step), step)],
            own_sem.at[q],
        ).wait()
        for h in range(2):
            for direction in (1, -1):
                send(q, h, 0, 0, 0, direction)
        for h in range(2):
            for direction in (1, -1):
                send(q, h, 0, 0, 1, direction)
        for h in range(2):
            share(q, h, 0, 0)

    hops = [[] for _ in range(5)]
    for fo in (0, -1, 1, 2):
        for so in (0, -1, 1, 2):
            hops[abs(fo) + abs(so)].append((fo, so))

    def pass_on(q, hop):
        for fo, so in hops[hop]:
            for h in range(2):
                arrived(q, h, fo, so)
                if so == 0:
                    if abs(fo) == 1 and first_way(q, h) == -fo:
                        send(q, h, fo, so, 0, -fo)
                    for direction in (1, -1):
                        send(q, h, fo, so, 1, direction)
                elif abs(so) == 1 and second_way(q, h, fo) == -so:
                    send(q, h, fo, so, 1, -so)
                share(q, h, fo, so)

    def prepare():
        load_v.wait()
        tile = 256

        def body(t, _):
            at_k = pl.multiple_of(t * tile, tile)
            block = v_mem[:, pl.ds(at_k, tile)].T
            hi = block.astype(jnp.bfloat16)
            lo = (block - hi.astype(jnp.float32)).astype(jnp.bfloat16)
            weights[pl.ds(at_k, tile), :] = hi
            weights[pl.ds(pl.multiple_of(depth + at_k, tile), tile), :] = lo
            weights[pl.ds(pl.multiple_of(2 * depth + at_k, tile), tile), :] = hi
            return 0

        lax.fori_loop(0, depth // tile, body, 0)

    ends = []
    total = 0
    for b in range(7):
        total = total + units_ref[b] * UNIT
        ends.append(total)

    def block_of(position):
        ids = jnp.zeros_like(position)
        for end in ends:
            ids = ids + (position >= end).astype(jnp.int32)
        return ids

    def multiply(q):
        group = 16
        row_block = block_of(z * depth + lax.broadcasted_iota(jnp.int32, (1, depth), 1))

        def split(g, _):
            first = pl.multiple_of(g * group, group)
            index = first + lax.broadcasted_iota(jnp.int32, (group, 1), 0)
            column = lax.div(index, step) * own + q * step + lax.rem(index, step)
            keep = block_of(START + column) == row_block
            block = jnp.where(keep, gathered[q, pl.ds(first, group), :], 0.0)
            hi = block.astype(jnp.bfloat16)
            lo = (block - hi.astype(jnp.float32)).astype(jnp.bfloat16)
            lhs[pl.ds(first, group), 0:depth] = hi
            lhs[pl.ds(first, group), depth:2 * depth] = hi
            lhs[pl.ds(first, group), 2 * depth:3 * depth] = lo
            return 0

        lax.fori_loop(0, width // group, split, 0)
        part[q] = jnp.dot(lhs[...], weights[...], preferred_element_type=jnp.float32)

    def chunk_rows(plane, start=0, size=chunk):
        return pl.ds(pl.multiple_of(plane * chunk + start, 8), size)

    def sum_copy(q, s, direction):
        if s == 1:
            start = 0 if direction == 1 else chunk // 2
            src = part.at[q, chunk_rows(shift(z, 4, planes), start, chunk // 2)]
            dst = (up_first if direction == 1 else down_first).at[q]
        else:
            src = part.at[q, chunk_rows(shift(z, direction * (5 - s), planes))]
            dst = (up_rest if direction == 1 else down_rest).at[q, s - 2]
        lane = 0 if direction == 1 else 1
        return pltpu.make_async_remote_copy(
            src_ref=src,
            dst_ref=dst,
            send_sem=sum_sent.at[q, lane, s - 1],
            recv_sem=sum_sem.at[q, lane, s - 1],
            device_id=up_id if direction == 1 else down_id,
            device_id_type=MESH,
        )

    def sum_first(q):
        for direction in (1, -1):
            sum_copy(q, 1, direction).start()

    def sum_next(q, s):
        for direction in (1, -1):
            sum_copy(q, s - 1, direction).wait_recv()
            got = up_first if direction == 1 else down_first
            target = shift(z, direction * (5 - s), planes)
            if s == 2:
                start = 0 if direction == 1 else chunk // 2
                where = chunk_rows(target, start, chunk // 2)
                part[q, where, :] = part[q, where, :] + got[q]
            else:
                got = up_rest if direction == 1 else down_rest
                where = chunk_rows(target)
                part[q, where, :] = part[q, where, :] + got[q, s - 3]
            sum_copy(q, s, direction).start()

    def sum_last(q):
        for direction in (1, -1):
            sum_copy(q, 4, direction).wait_recv()
        total = part[q, chunk_rows(z), :] + up_rest[q, 2] + down_rest[q, 2]
        for i in range(per_keep):
            o_ref[i * own + q * step:i * own + (q + 1) * step, :] = total[i * step:(i + 1) * step, :]

    def sums(q, s):
        if 0 <= q < PHASES:
            if s == 1:
                sum_first(q)
            elif s == 5:
                sum_last(q)
            else:
                sum_next(q, s)

    def drain(q):
        n = 2 * (RINGS * RINGS - 1)
        ref = gathered.at[q, pl.ds(0, n // 2 * step)]
        pltpu.make_async_copy(ref, ref, gather_sent.at[q]).wait()
        ref = gathered.at[q, pl.ds(0, RINGS * RINGS * step)]
        pltpu.make_async_copy(ref, ref, mate_sent.at[q]).wait()
        for s in range(1, 5):
            for direction in (1, -1):
                sum_copy(q, s, direction).wait_send()

    def mate_arrived(q):
        ref = gathered.at[q, pl.ds(0, RINGS * RINGS * step)]
        pltpu.make_async_copy(ref, ref, mate_sem.at[q]).wait()

    for q in range(AHEAD):
        level0(q)
    prepare()
    for tick in range(PHASES + 3 + LAG):
        for hop in HOP_ORDER:
            q = tick - (hop - 1)
            if 0 <= q < PHASES:
                pass_on(q, hop)
        if tick + AHEAD < PHASES:
            level0(tick + AHEAD)
        done = tick - 3
        for s in (5, 4, 3, 2):
            sums(done - s + 1 - LAG, s)
        if 0 <= done - LAG < PHASES:
            mate_arrived(done - LAG)
            multiply(done - LAG)
            sums(done - LAG, 1)
    for extra in range(1, 4):
        for s in (5, 4, 3, 2):
            sums(PHASES - 1 + extra - s + 1, s)
    for q in range(PHASES):
        drain(q)
    sums(PHASES - 1, 5)


def solution(mesh):
    devices, planes = mesh.shape["row"], mesh.shape["col"]

    def body(vectors, basis, block_units):
        rows, depth = vectors.shape
        own = basis.shape[1]
        step = own // PHASES
        width = step * devices
        chunk = width // planes
        f32, bf16 = jnp.float32, jnp.bfloat16
        summed = pl.pallas_call(
            functools.partial(kernel, (rows, depth, own, devices, planes)),
            out_shape=jax.ShapeDtypeStruct((own * devices // planes, rows), f32),
            in_specs=[
                pl.BlockSpec(memory_space=pltpu.SMEM),
                pl.BlockSpec(memory_space=pl.ANY),
                pl.BlockSpec(memory_space=pl.ANY),
            ],
            out_specs=pl.BlockSpec(memory_space=pltpu.VMEM),
            scratch_shapes=[
                pltpu.VMEM((PHASES, width, depth), f32),
                pltpu.VMEM((rows, depth), f32),
                pltpu.VMEM((3 * depth, rows), bf16),
                pltpu.VMEM((width, 3 * depth), bf16),
                pltpu.VMEM((PHASES, width, rows), f32),
                pltpu.VMEM((PHASES, chunk // 2, rows), f32),
                pltpu.VMEM((PHASES, 3, chunk, rows), f32),
                pltpu.VMEM((PHASES, chunk // 2, rows), f32),
                pltpu.VMEM((PHASES, 3, chunk, rows), f32),
                pltpu.SemaphoreType.DMA,
                pltpu.SemaphoreType.DMA((PHASES,)),
                pltpu.SemaphoreType.DMA((PHASES, 2, RINGS * RINGS)),
                pltpu.SemaphoreType.DMA((PHASES,)),
                pltpu.SemaphoreType.DMA((PHASES,)),
                pltpu.SemaphoreType.DMA((PHASES,)),
                pltpu.SemaphoreType.DMA((PHASES, 2, 4)),
                pltpu.SemaphoreType.DMA((PHASES, 2, 4)),
            ],
            compiler_params=pltpu.CompilerParams(
                collective_id=0, has_side_effects=True, vmem_limit_bytes=63 * 1024 * 1024
            ),
            cost_estimate=pl.CostEstimate(
                flops=6 * rows * depth * own * devices, bytes_accessed=4 * rows * depth, transcendentals=0
            ),
        )(block_units, vectors, basis.T)
        return summed.T

    return jax.shard_map(
        body,
        mesh=mesh,
        in_specs=(P("row", "col"), P("col", "row"), P()),
        out_specs=P("row", "col"),
        check_vma=False,
    )
```

```python
import functools

import jax
import jax.numpy as jnp
from jax import lax
from jax.experimental import pallas as pl
from jax.experimental.pallas import tpu as pltpu
from jax.sharding import PartitionSpec as P

MESH = pl.DeviceIdType.MESH
UNIT = 256
START = 7168
RINGS = 4
SIZES = (16, 16, 16, 16)
ORDER = (
    (0, 0, 0, 0, 0), (2, 0, 0, 0, 0), (0, 1, 0, 0, 0), (1, 0, 1, -1, 0), (1, 0, 1, 1, 0), (1, 0, 0, -1, 0), (1, 0, 0, 1, 0),
    (1, 0, 0, 0, -1), (1, 0, 0, 0, 1), (1, 0, 1, 0, -1), (1, 0, 1, 0, 1), (1, 1, 1, -1, 0), (1, 1, 1, 1, 0),
    (1, 1, 0, -1, 0), (1, 1, 0, 1, 0), (1, 1, 0, 0, -1), (1, 1, 0, 0, 1), (1, 1, 1, 0, -1), (1, 1, 1, 0, 1),
    (1, 0, 0, -1, -1), (1, 0, 1, 2, 0), (1, 0, 1, -1, -1), (1, 0, 1, -1, 1), (1, 0, 0, 1, -1), (1, 0, 0, -1, 1),
    (1, 0, 1, 1, -1), (1, 0, 1, 1, 1), (1, 0, 0, 0, 2), (1, 0, 0, 1, 1), (1, 0, 0, 2, 0), (1, 1, 1, -1, 1), (3, 0, 0, 0, 0),
    (1, 0, 1, 0, 2), (1, 1, 1, 2, 0), (1, 1, 0, -1, 1), (1, 1, 1, 1, 1), (1, 1, 0, -1, -1), (1, 1, 0, 1, 1),
    (1, 1, 1, -1, -1), (1, 1, 0, 2, 0), (1, 1, 0, 1, -1), (1, 1, 0, 0, 2), (1, 1, 1, 1, -1), (1, 1, 1, 0, 2),
    (4, 0, 0, 2, 0), (1, 0, 0, -1, 2), (1, 0, 0, 1, 2), (1, 0, 1, 2, -1), (1, 0, 1, 2, 1), (3, 1, 0, 0, 0), (0, 2, 0, 0, 0),
    (1, 0, 0, 2, -1), (1, 0, 0, 2, 1), (1, 0, 1, -1, 2), (1, 0, 1, 1, 2), (3, 0, -1, 0, 0), (1, 1, 0, 2, -1),
    (1, 1, 0, -1, 2), (1, 1, 1, 2, -1), (1, 1, 1, -1, 2), (3, 0, 1, 0, 0), (4, 0, 0, 3, 0), (1, 1, 0, 1, 2),
    (1, 1, 0, 2, 1), (1, 1, 1, 2, 1), (1, 1, 1, 1, 2), (3, 1, -1, 0, 0), (0, 3, 0, 0, 0), (4, 1, 0, 2, 0), (1, 0, 1, 2, 2),
    (1, 2, 1, -1, 0), (1, 2, 1, 1, 0), (4, 0, -1, 2, 0), (1, 2, 0, -1, 0), (3, 1, 1, 0, 0), (4, 0, 1, 2, 0),
    (1, 2, 0, 0, -1), (1, 2, 0, 0, 1), (1, 2, 1, 0, -1), (1, 2, 0, 1, 0), (4, 0, 0, 4, 0), (1, 1, 0, 2, 2), (1, 0, 0, 2, 2),
    (1, 1, 1, 2, 2), (1, 2, 1, 0, 1), (4, 1, -1, 2, 0), (4, 1, 0, 3, 0), (1, 3, 1, -1, 0), (1, 3, 1, 1, 0),
    (1, 3, 0, -1, 0), (1, 3, 0, 1, 0), (3, 0, 2, 0, 0), (4, 0, -1, 3, 0), (4, 1, 1, 2, 0), (4, 0, 1, 3, 0),
    (1, 3, 0, 0, -1), (1, 3, 0, 0, 1), (1, 3, 1, 0, -1), (1, 3, 1, 0, 1), (3, 1, 2, 0, 0), (4, 0, 0, 5, 0),
    (4, 1, -1, 3, 0), (1, 2, 1, 2, 0), (1, 2, 0, -1, -1), (1, 2, 1, -1, -1), (1, 2, 1, -1, 1), (4, 1, 0, 4, 0),
    (1, 2, 0, 0, 2), (1, 2, 0, -1, 1), (1, 2, 1, 1, -1), (1, 2, 1, 1, 1), (4, 0, 2, 2, 0), (3, 2, 0, 0, 0),
    (4, 0, -1, 4, 0), (4, 1, 1, 3, 0), (1, 2, 0, 1, -1), (4, 0, 1, 4, 0), (4, 1, 2, 2, 0), (1, 2, 0, 1, 1), (1, 2, 0, 2, 0),
    (1, 2, 1, 0, 2), (1, 3, 1, 2, 0), (1, 3, 1, -1, 1), (1, 3, 0, -1, 1), (1, 3, 1, 1, 1), (4, 1, -1, 4, 0),
    (1, 3, 0, -1, -1), (1, 3, 0, 1, 1), (1, 3, 1, -1, -1), (1, 3, 0, 2, 0), (4, 1, 0, 5, 0), (4, 0, 2, 3, 0),
    (4, 2, 0, 2, 0), (1, 3, 0, 0, 2), (1, 3, 0, 1, -1), (1, 3, 1, 1, -1), (1, 3, 1, 0, 2), (4, 0, -1, 5, 0),
    (1, 2, 0, -1, 2), (1, 2, 0, 1, 2), (1, 2, 1, 2, -1), (1, 2, 1, 2, 1), (3, 3, 0, 0, 0), (4, 1, 1, 4, 0), (4, 0, 1, 5, 0),
    (1, 2, 0, 2, -1), (1, 2, 0, 2, 1), (1, 2, 1, -1, 2), (1, 2, 1, 1, 2), (3, 2, -1, 0, 0), (4, 1, 2, 3, 0),
    (4, 1, -1, 5, 0), (1, 3, 0, -1, 2), (1, 3, 1, 2, -1), (4, 0, 2, 4, 0), (1, 3, 1, 2, 1), (1, 3, 0, 2, -1),
    (3, 2, 1, 0, 0), (4, 2, 0, 3, 0), (4, 3, 0, 2, 0), (1, 3, 0, 1, 2), (1, 3, 0, 2, 1), (1, 3, 1, 1, 2), (1, 3, 1, -1, 2),
    (3, 3, -1, 0, 0), (4, 1, 1, 5, 0), (4, 2, -1, 2, 0), (1, 2, 0, 2, 2), (1, 2, 1, 2, 2), (3, 3, 1, 0, 0), (4, 1, 2, 4, 0),
    (1, 3, 1, 2, 2), (4, 2, 1, 2, 0), (4, 0, 2, 5, 0), (1, 3, 0, 2, 2), (3, 2, 2, 0, 0), (4, 2, 0, 4, 0), (3, 3, 2, 0, 0),
    (4, 3, -1, 2, 0), (4, 3, 0, 3, 0), (4, 2, -1, 3, 0), (4, 3, 1, 2, 0), (4, 1, 2, 5, 0), (4, 2, 2, 2, 0), (4, 2, 1, 3, 0),
    (4, 2, 0, 5, 0), (4, 3, 2, 2, 0), (4, 3, -1, 3, 0), (4, 3, 0, 4, 0), (4, 2, -1, 4, 0), (4, 3, 1, 3, 0), (4, 2, 2, 3, 0),
    (4, 2, 1, 4, 0), (4, 3, 2, 3, 0), (4, 3, -1, 4, 0), (4, 3, 0, 5, 0), (4, 2, -1, 5, 0), (4, 3, 1, 4, 0), (4, 2, 2, 4, 0),
    (4, 2, 1, 5, 0), (4, 3, 2, 4, 0), (4, 3, -1, 5, 0), (4, 3, 1, 5, 0), (4, 2, 2, 5, 0), (4, 3, 2, 5, 0),
)


def kernel(dims, units_ref, v_hbm, bt_hbm, o_ref, gathered, v_mem, weights, lhs, part, brought, local_sem, own_sem,
           gather_sem, gather_sent, mate_sem, mate_sent, sum_sem, sum_sent):
    rows, depth, own, planes = dims
    half = depth // 2
    offsets = [sum(SIZES[:q]) for q in range(len(SIZES))]

    me = lax.axis_index("row")
    z = lax.axis_index("col")
    core = lax.rem(me, 2)
    x = lax.rem(lax.div(me, 2), RINGS)
    y = lax.div(me, 2 * RINGS)

    def shift(c, by, n):
        return lax.rem(c + (by % n), n)

    def device(xx, yy):
        return (yy * RINGS + xx) * 2 + core

    mate_id = (me + 1 - 2 * core, z)
    neighbour = {
        ("x", 1): (device(shift(x, 1, RINGS), y), z),
        ("x", -1): (device(shift(x, -1, RINGS), y), z),
        ("y", 1): (device(x, shift(y, 1, RINGS)), z),
        ("y", -1): (device(x, shift(y, -1, RINGS)), z),
    }
    along_z = {1: (me, shift(z, 1, planes)), -1: (me, shift(z, -1, planes))}
    axes = (("x", "y"), ("y", "x"))

    def slot(q, xx, yy):
        step = SIZES[q]
        return pl.multiple_of(offsets[q] * 2 * RINGS * RINGS + ((xx * RINGS + yy) * 2 + core) * step, 8)

    def own_copy(q):
        step = SIZES[q]
        return pltpu.make_async_copy(
            bt_hbm.at[pl.ds(offsets[q], step)], gathered.at[pl.ds(slot(q, x, y), step)], own_sem.at[q]
        )

    for q in range(len(SIZES)):
        own_copy(q).start()
    load_v = pltpu.make_async_copy(v_hbm, v_mem, local_sem)
    load_v.start()

    barrier = pltpu.get_barrier_semaphore()
    for other in (*neighbour.values(), mate_id, *along_z.values()):
        pl.semaphore_signal(barrier, inc=1, device_id=other, device_id_type=MESH)
    pl.semaphore_wait(barrier, 7)

    def piece(q, h, fo, so):
        dx, dy = (fo, so) if h == 0 else (so, fo)
        first = slot(q, shift(x, dx, RINGS), shift(y, dy, RINGS))
        return gathered.at[pl.ds(first, SIZES[q]), pl.ds(h * half, half)]

    def send(q, h, fo, so, which, direction):
        ref = piece(q, h, fo, so)
        nfo, nso = (fo - direction, so) if which == 0 else (fo, so - direction)
        pltpu.make_async_remote_copy(
            src_ref=ref,
            dst_ref=ref,
            send_sem=gather_sent,
            recv_sem=gather_sem.at[q, h, (nfo % RINGS) * RINGS + nso % RINGS],
            device_id=neighbour[axes[h][which], direction],
            device_id_type=MESH,
        ).start()

    def share(q, h, fo, so):
        ref = piece(q, h, fo, so)
        dx = (fo if h == 0 else so) % RINGS
        pltpu.make_async_remote_copy(
            src_ref=ref,
            dst_ref=ref,
            send_sem=mate_sent,
            recv_sem=mate_sem.at[q, dx],
            device_id=mate_id,
            device_id_type=MESH,
        ).start()

    def begin(q):
        own_copy(q).wait()
        for h in (1, 0):
            for direction in (1, -1):
                send(q, h, 0, 0, 1 - h, direction)
        for h in (0, 1):
            for direction in (1, -1):
                send(q, h, 0, 0, h, direction)
        for h in range(2):
            share(q, h, 0, 0)

    def pass_on(q, h, fo, so):
        ref = piece(q, h, fo, so)
        pltpu.make_async_copy(ref, ref, gather_sem.at[q, h, (fo % RINGS) * RINGS + so % RINGS]).wait()
        if so == 0:
            if abs(fo) == 1 and (1 if (q + h) % 2 == 0 else -1) == -fo:
                send(q, h, fo, so, 0, -fo)
            for direction in (1, -1):
                send(q, h, fo, so, 1, direction)
        elif abs(so) == 1 and (1 if (q + fo // 2 + fo) % 2 == 0 else -1) == -so:
            send(q, h, fo, so, 1, -so)
        share(q, h, fo, so)

    def prepare():
        load_v.wait()
        tile = 256

        def body(t, _):
            at_k = pl.multiple_of(t * tile, tile)
            block = v_mem[:, pl.ds(at_k, tile)].T
            hi = block.astype(jnp.bfloat16)
            lo = (block - hi.astype(jnp.float32)).astype(jnp.bfloat16)
            weights[pl.ds(at_k, tile), :] = hi
            weights[pl.ds(pl.multiple_of(depth + at_k, tile), tile), :] = lo
            weights[pl.ds(pl.multiple_of(2 * depth + at_k, tile), tile), :] = hi
            return 0

        lax.fori_loop(0, depth // tile, body, 0)

    ends = []
    total = 0
    for b in range(7):
        total = total + units_ref[b] * UNIT
        ends.append(total)

    def block_of(position):
        ids = jnp.zeros_like(position)
        for end in ends:
            ids = ids + (position >= end).astype(jnp.int32)
        return ids

    def group_first(q, dx):
        step = SIZES[q]
        return pl.multiple_of(
            offsets[q] * 2 * RINGS * RINGS + shift(x, dx, RINGS) * (2 * RINGS * step), 2 * RINGS * 8
        )

    def multiply(q, dx):
        step = SIZES[q]
        width = 2 * RINGS * step
        first = group_first(q, dx)
        ref = gathered.at[pl.ds(0, RINGS * step)]
        pltpu.make_async_copy(ref, ref, mate_sem.at[q, dx % RINGS]).wait()
        xx = shift(x, dx, RINGS)
        row_block = block_of(z * depth + lax.broadcasted_iota(jnp.int32, (1, depth), 1))
        batch = 16

        def split(g, _):
            at_row = pl.multiple_of(g * batch, batch)
            index = at_row + lax.broadcasted_iota(jnp.int32, (batch, 1), 0)
            chip = lax.div(index, 2 * step) * RINGS + xx
            owner = chip * 2 + lax.rem(lax.div(index, step), 2)
            column = owner * own + offsets[q] + lax.rem(index, step)
            keep = block_of(START + column) == row_block
            block = jnp.where(keep, gathered[pl.ds(pl.multiple_of(first + at_row, batch), batch), :], 0.0)
            hi = block.astype(jnp.bfloat16)
            lo = (block - hi.astype(jnp.float32)).astype(jnp.bfloat16)
            lhs[pl.ds(at_row, batch), 0:depth] = hi
            lhs[pl.ds(at_row, batch), depth:2 * depth] = hi
            lhs[pl.ds(at_row, batch), 2 * depth:3 * depth] = lo
            return 0

        lax.fori_loop(0, width // batch, split, 0)
        across = 256

        def product(m, _):
            lanes = pl.ds(pl.multiple_of(m * across, across), across)
            part[pl.ds(first, width), lanes] = jnp.dot(
                lhs[0:width, :], weights[:, lanes], preferred_element_type=jnp.float32
            )
            return 0

        lax.fori_loop(0, rows // across, product, 0)

    def add_up(q, dx, s):
        step = SIZES[q]
        chunk = 2 * step
        xx = shift(x, dx, RINGS)
        side = lax.div(xx, 2)
        odd = lax.rem(z + side, 2)
        near = lax.rem(lax.div(z - side + 9, 2), RINGS)
        first = group_first(q, dx)
        slot_first = offsets[q] * 2 * RINGS + (dx % RINGS) * chunk

        def rows_of(j, start, size):
            return pl.ds(pl.multiple_of(first + shift(near, j, RINGS) * chunk + start, 8), size)

        def wait_for(lane, slot_at, size):
            ref = brought.at[lane, slot_at, pl.ds(slot_first, size)]
            pltpu.make_async_copy(ref, ref, sum_sem.at[q, dx % RINGS, lane * 2 + slot_at]).wait()

        def send_on(lane, slot_at, src, size):
            pltpu.make_async_remote_copy(
                src_ref=part.at[src],
                dst_ref=brought.at[lane, slot_at, pl.ds(slot_first, size)],
                send_sem=sum_sent,
                recv_sem=sum_sem.at[q, dx % RINGS, lane * 2 + slot_at],
                device_id=along_z[1 - 2 * lane],
                device_id_type=MESH,
            ).start()

        @pl.when(odd == (s + 1) % 2)
        def _():
            if s == 5:
                for lane in range(2):
                    wait_for(lane, 1, chunk)
                where = pl.ds(slot_first, chunk)
                final = part[rows_of(0, 0, chunk), :] + brought[0, 1, where, :] + brought[1, 1, where, :]
                for i in range(2):
                    to = pl.multiple_of(lax.rem(xx, 2) * (2 * own) + i * own + offsets[q], 8)
                    o_ref[pl.ds(to, step), :] = final[i * step:(i + 1) * step, :]
                return
            for lane in range(2):
                start = lane * step
                j = {1: (2, 2), 2: (1, -2), 3: (1, -1), 4: (0, -1)}[s][lane]
                if s == 1:
                    send_on(lane, 0, rows_of(j, start, step), step)
                    continue
                if s == 2:
                    wait_for(lane, 0, step)
                    where = rows_of(j, start, step)
                    part[where, :] = part[where, :] + brought[lane, 0, pl.ds(slot_first, step), :]
                else:
                    wait_for(lane, s - 3, chunk)
                    where = rows_of(j, 0, chunk)
                    part[where, :] = part[where, :] + brought[lane, s - 3, pl.ds(slot_first, chunk), :]
                send_on(lane, 0 if s == 2 else 1, rows_of(j, 0, chunk), chunk)

    for op, q, a, b, c in ORDER:
        if op == 0:
            begin(q)
        elif op == 1:
            pass_on(q, a, b, c)
        elif op == 2:
            prepare()
        elif op == 3:
            multiply(q, a)
            add_up(q, a, 1)
        else:
            add_up(q, a, b)

    ref = gathered.at[pl.ds(0, (RINGS * RINGS - 1) * own)]
    pltpu.make_async_copy(ref, ref, gather_sent).wait()
    ref = gathered.at[pl.ds(0, RINGS * RINGS * own)]
    pltpu.make_async_copy(ref, ref, mate_sent).wait()
    ref = part.at[pl.ds(0, 28 * own)]
    pltpu.make_async_copy(ref, ref, sum_sent).wait()


def solution(mesh):
    devices, planes = mesh.shape["row"], mesh.shape["col"]
    phases = len(SIZES)

    def body(vectors, basis, block_units):
        rows, depth = vectors.shape
        own = basis.shape[1]
        f32, bf16 = jnp.float32, jnp.bfloat16
        dma = pltpu.SemaphoreType.DMA
        summed = pl.pallas_call(
            functools.partial(kernel, (rows, depth, own, planes)),
            out_shape=jax.ShapeDtypeStruct((own * devices // planes, rows), f32),
            in_specs=[
                pl.BlockSpec(memory_space=pltpu.SMEM),
                pl.BlockSpec(memory_space=pl.ANY),
                pl.BlockSpec(memory_space=pl.ANY),
            ],
            out_specs=pl.BlockSpec(memory_space=pltpu.VMEM),
            scratch_shapes=[
                pltpu.VMEM((own * devices, depth), f32),
                pltpu.VMEM((rows, depth), f32),
                pltpu.VMEM((3 * depth, rows), bf16),
                pltpu.VMEM((2 * RINGS * max(SIZES), 3 * depth), bf16),
                pltpu.VMEM((own * devices, rows), f32),
                pltpu.VMEM((2, 2, 2 * RINGS * own, rows), f32),
                dma,
                dma((phases,)),
                dma((phases, 2, RINGS * RINGS)),
                dma,
                dma((phases, RINGS)),
                dma,
                dma((phases, RINGS, 4)),
                dma,
            ],
            compiler_params=pltpu.CompilerParams(
                collective_id=0, has_side_effects=True, vmem_limit_bytes=63 * 1024 * 1024
            ),
            cost_estimate=pl.CostEstimate(
                flops=6 * rows * depth * own * devices, bytes_accessed=4 * rows * depth, transcendentals=0
            ),
        )(block_units, vectors, basis.T)
        return summed.T

    return jax.shard_map(
        body,
        mesh=mesh,
        in_specs=(P("row", "col"), P("col", "row"), P()),
        out_specs=P("row", "col"),
        check_vma=False,
    )
```

```python
import functools

import jax
import jax.numpy as jnp
from jax import lax
from jax.experimental import pallas as pl
from jax.experimental.pallas import tpu as pltpu
from jax.sharding import PartitionSpec as P

MESH = pl.DeviceIdType.MESH
UNIT = 256
START = 7168
RINGS = 4
SIZES = (16, 16, 16, 16)
ORDER = (
    (0, 0, 0, 0, 0), (2, 0, 0, 0, 0), (0, 1, 0, 0, 0), (1, 0, 1, -1, 0), (1, 0, 1, 1, 0), (1, 0, 0, -1, 0), (1, 0, 0, 1, 0),
    (1, 0, 0, 0, -1), (1, 0, 0, 0, 1), (1, 0, 1, 0, -1), (1, 0, 1, 0, 1), (1, 1, 1, -1, 0), (1, 1, 1, 1, 0),
    (1, 1, 0, -1, 0), (1, 1, 0, 1, 0), (1, 1, 0, 0, -1), (1, 1, 0, 0, 1), (1, 1, 1, 0, -1), (1, 1, 1, 0, 1),
    (1, 0, 0, -1, -1), (1, 0, 1, 2, 0), (1, 0, 1, -1, -1), (1, 0, 1, -1, 1), (1, 0, 0, 1, -1), (1, 0, 0, -1, 1),
    (1, 0, 1, 1, -1), (1, 0, 1, 1, 1), (1, 0, 0, 0, 2), (1, 0, 0, 1, 1), (1, 0, 0, 2, 0), (1, 1, 1, -1, 1), (3, 0, 0, 0, 0),
    (1, 0, 1, 0, 2), (1, 1, 1, 2, 0), (1, 1, 0, -1, 1), (1, 1, 1, 1, 1), (1, 1, 0, -1, -1), (1, 1, 0, 1, 1),
    (1, 1, 1, -1, -1), (1, 1, 0, 2, 0), (1, 1, 0, 1, -1), (1, 1, 0, 0, 2), (1, 1, 1, 1, -1), (1, 1, 1, 0, 2),
    (1, 0, 0, -1, 2), (1, 0, 0, 1, 2), (1, 0, 1, 2, -1), (1, 0, 1, 2, 1), (3, 1, 0, 0, 0), (4, 0, 0, 2, 0), (0, 2, 0, 0, 0),
    (1, 0, 0, 2, -1), (1, 0, 0, 2, 1), (1, 0, 1, -1, 2), (1, 0, 1, 1, 2), (3, 0, -1, 0, 0), (1, 1, 0, -1, 2),
    (1, 1, 1, 2, -1), (1, 1, 0, 2, -1), (1, 1, 1, -1, 2), (3, 0, 1, 0, 0), (1, 1, 0, 1, 2), (1, 1, 0, 2, 1),
    (1, 1, 1, 1, 2), (1, 1, 1, 2, 1), (3, 1, -1, 0, 0), (4, 1, 0, 2, 0), (0, 3, 0, 0, 0), (1, 0, 1, 2, 2), (1, 2, 1, -1, 0),
    (1, 2, 1, 1, 0), (1, 2, 0, -1, 0), (3, 1, 1, 0, 0), (4, 0, 0, 3, 0), (4, 0, -1, 2, 0), (1, 2, 0, 0, -1),
    (1, 2, 0, 0, 1), (1, 2, 1, 0, -1), (1, 2, 0, 1, 0), (4, 0, 1, 2, 0), (1, 1, 0, 2, 2), (1, 0, 0, 2, 2), (1, 1, 1, 2, 2),
    (1, 2, 1, 0, 1), (4, 1, -1, 2, 0), (1, 3, 1, -1, 0), (1, 3, 1, 1, 0), (1, 3, 0, -1, 0), (1, 3, 0, 1, 0),
    (3, 0, 2, 0, 0), (4, 1, 0, 3, 0), (4, 1, 1, 2, 0), (1, 3, 0, 0, -1), (1, 3, 0, 0, 1), (1, 3, 1, 0, -1), (1, 3, 1, 0, 1),
    (3, 1, 2, 0, 0), (4, 0, 0, 4, 0), (1, 2, 1, 2, 0), (1, 2, 0, -1, -1), (4, 0, -1, 3, 0), (1, 2, 1, -1, -1),
    (1, 2, 1, -1, 1), (4, 0, 1, 3, 0), (1, 2, 0, 0, 2), (1, 2, 0, -1, 1), (1, 2, 1, 1, -1), (1, 2, 1, 1, 1),
    (4, 1, -1, 3, 0), (4, 0, 2, 2, 0), (1, 2, 0, 1, -1), (1, 2, 0, 1, 1), (1, 2, 0, 2, 0), (1, 3, 1, -1, 1),
    (3, 2, 0, 0, 0), (4, 1, 0, 4, 0), (1, 2, 1, 0, 2), (1, 3, 1, 2, 0), (1, 3, 0, -1, 1), (1, 3, 1, 1, 1), (4, 1, 1, 3, 0),
    (4, 1, 2, 2, 0), (4, 0, 0, 5, 0), (1, 3, 0, -1, -1), (1, 3, 0, 1, 1), (1, 3, 1, -1, -1), (1, 3, 0, 2, 0),
    (4, 0, -1, 4, 0), (4, 0, 1, 4, 0), (1, 3, 0, 0, 2), (1, 3, 0, 1, -1), (1, 3, 1, 1, -1), (1, 3, 1, 0, 2),
    (4, 1, -1, 4, 0), (4, 2, 0, 2, 0), (4, 0, 2, 3, 0), (1, 2, 0, -1, 2), (1, 2, 0, 1, 2), (1, 2, 1, 2, -1),
    (1, 2, 1, 2, 1), (3, 3, 0, 0, 0), (4, 1, 0, 5, 0), (1, 2, 0, 2, -1), (1, 2, 0, 2, 1), (4, 1, 1, 4, 0), (1, 2, 1, -1, 2),
    (1, 2, 1, 1, 2), (3, 2, -1, 0, 0), (4, 1, 2, 3, 0), (4, 0, -1, 5, 0), (1, 3, 0, -1, 2), (1, 3, 1, 2, -1),
    (1, 3, 0, 2, -1), (1, 3, 1, -1, 2), (3, 2, 1, 0, 0), (4, 0, 1, 5, 0), (4, 1, -1, 5, 0), (1, 3, 0, 1, 2),
    (1, 3, 1, 2, 1), (1, 3, 0, 2, 1), (1, 3, 1, 1, 2), (3, 3, -1, 0, 0), (4, 2, 0, 3, 0), (4, 3, 0, 2, 0), (4, 0, 2, 4, 0),
    (1, 2, 0, 2, 2), (1, 2, 1, 2, 2), (3, 3, 1, 0, 0), (4, 1, 1, 5, 0), (4, 2, -1, 2, 0), (1, 3, 1, 2, 2), (1, 3, 0, 2, 2),
    (3, 2, 2, 0, 0), (4, 1, 2, 4, 0), (4, 2, 1, 2, 0), (3, 3, 2, 0, 0), (4, 3, -1, 2, 0), (4, 2, 0, 4, 0), (4, 3, 0, 3, 0),
    (4, 3, 1, 2, 0), (4, 0, 2, 5, 0), (4, 2, 2, 2, 0), (4, 2, -1, 3, 0), (4, 1, 2, 5, 0), (4, 3, 2, 2, 0), (4, 2, 1, 3, 0),
    (4, 3, -1, 3, 0), (4, 2, 0, 5, 0), (4, 3, 0, 4, 0), (4, 3, 1, 3, 0), (4, 2, 2, 3, 0), (4, 2, -1, 4, 0), (4, 3, 2, 3, 0),
    (4, 2, 1, 4, 0), (4, 3, -1, 4, 0), (4, 3, 0, 5, 0), (4, 3, 1, 4, 0), (4, 2, 2, 4, 0), (4, 2, -1, 5, 0), (4, 3, 2, 4, 0),
    (4, 2, 1, 5, 0), (4, 3, -1, 5, 0), (4, 3, 1, 5, 0), (4, 2, 2, 5, 0), (4, 3, 2, 5, 0),
)


def kernel(dims, units_ref, v_hbm, bt_hbm, o_ref, gathered, v_mem, weights, lhs, part, brought, local_sem, own_sem,
           gather_sem, gather_sent, mate_sem, mate_sent, sum_sem, sum_sent):
    rows, depth, own, planes = dims
    half = depth // 2
    offsets = [sum(SIZES[:q]) for q in range(len(SIZES))]

    me = lax.axis_index("row")
    z = lax.axis_index("col")
    core = lax.rem(me, 2)
    x = lax.rem(lax.div(me, 2), RINGS)
    y = lax.div(me, 2 * RINGS)

    def shift(c, by, n):
        return lax.rem(c + (by % n), n)

    def device(xx, yy):
        return (yy * RINGS + xx) * 2 + core

    mate_id = (me + 1 - 2 * core, z)
    neighbour = {
        ("x", 1): (device(shift(x, 1, RINGS), y), z),
        ("x", -1): (device(shift(x, -1, RINGS), y), z),
        ("y", 1): (device(x, shift(y, 1, RINGS)), z),
        ("y", -1): (device(x, shift(y, -1, RINGS)), z),
    }
    along_z = {1: (me, shift(z, 1, planes)), -1: (me, shift(z, -1, planes))}
    axes = (("x", "y"), ("y", "x"))

    def slot(q, xx, yy):
        step = SIZES[q]
        return pl.multiple_of(offsets[q] * 2 * RINGS * RINGS + ((xx * RINGS + yy) * 2 + core) * step, 8)

    def own_copy(q):
        step = SIZES[q]
        return pltpu.make_async_copy(
            bt_hbm.at[pl.ds(offsets[q], step)], gathered.at[pl.ds(slot(q, x, y), step)], own_sem.at[q]
        )

    for q in range(len(SIZES)):
        own_copy(q).start()
    load_v = pltpu.make_async_copy(v_hbm, v_mem, local_sem)
    load_v.start()

    barrier = pltpu.get_barrier_semaphore()
    for other in (*neighbour.values(), mate_id, *along_z.values()):
        pl.semaphore_signal(barrier, inc=1, device_id=other, device_id_type=MESH)
    pl.semaphore_wait(barrier, 7)

    def piece(q, h, fo, so):
        dx, dy = (fo, so) if h == 0 else (so, fo)
        first = slot(q, shift(x, dx, RINGS), shift(y, dy, RINGS))
        return gathered.at[pl.ds(first, SIZES[q]), pl.ds(h * half, half)]

    def send(q, h, fo, so, which, direction):
        ref = piece(q, h, fo, so)
        nfo, nso = (fo - direction, so) if which == 0 else (fo, so - direction)
        pltpu.make_async_remote_copy(
            src_ref=ref,
            dst_ref=ref,
            send_sem=gather_sent,
            recv_sem=gather_sem.at[q, h, (nfo % RINGS) * RINGS + nso % RINGS],
            device_id=neighbour[axes[h][which], direction],
            device_id_type=MESH,
        ).start()

    def share(q, h, fo, so):
        ref = piece(q, h, fo, so)
        dx = (fo if h == 0 else so) % RINGS
        pltpu.make_async_remote_copy(
            src_ref=ref,
            dst_ref=ref,
            send_sem=mate_sent,
            recv_sem=mate_sem.at[q, dx],
            device_id=mate_id,
            device_id_type=MESH,
        ).start()

    def begin(q):
        own_copy(q).wait()
        for h in (1, 0):
            for direction in (1, -1):
                send(q, h, 0, 0, 1 - h, direction)
        for h in (0, 1):
            for direction in (1, -1):
                send(q, h, 0, 0, h, direction)
        for h in range(2):
            share(q, h, 0, 0)

    def pass_on(q, h, fo, so):
        ref = piece(q, h, fo, so)
        pltpu.make_async_copy(ref, ref, gather_sem.at[q, h, (fo % RINGS) * RINGS + so % RINGS]).wait()
        if so == 0:
            if abs(fo) == 1 and (1 if (q + h) % 2 == 0 else -1) == -fo:
                send(q, h, fo, so, 0, -fo)
            for direction in (1, -1):
                send(q, h, fo, so, 1, direction)
        elif abs(so) == 1 and (1 if (q + fo // 2 + fo) % 2 == 0 else -1) == -so:
            send(q, h, fo, so, 1, -so)
        share(q, h, fo, so)

    def prepare():
        load_v.wait()
        tile = 256

        def body(t, _):
            at_k = pl.multiple_of(t * tile, tile)
            block = v_mem[:, pl.ds(at_k, tile)].T
            hi = block.astype(jnp.bfloat16)
            lo = (block - hi.astype(jnp.float32)).astype(jnp.bfloat16)
            weights[pl.ds(at_k, tile), :] = hi
            weights[pl.ds(pl.multiple_of(depth + at_k, tile), tile), :] = lo
            weights[pl.ds(pl.multiple_of(2 * depth + at_k, tile), tile), :] = hi
            return 0

        lax.fori_loop(0, depth // tile, body, 0)

    ends = []
    total = 0
    for b in range(7):
        total = total + units_ref[b] * UNIT
        ends.append(total)

    def block_of(position):
        ids = jnp.zeros_like(position)
        for end in ends:
            ids = ids + (position >= end).astype(jnp.int32)
        return ids

    def group_first(q, dx):
        step = SIZES[q]
        return pl.multiple_of(
            offsets[q] * 2 * RINGS * RINGS + shift(x, dx, RINGS) * (2 * RINGS * step), 2 * RINGS * 8
        )

    def multiply(q, dx):
        step = SIZES[q]
        width = 2 * RINGS * step
        first = group_first(q, dx)
        ref = gathered.at[pl.ds(0, RINGS * step)]
        pltpu.make_async_copy(ref, ref, mate_sem.at[q, dx % RINGS]).wait()
        xx = shift(x, dx, RINGS)
        row_block = block_of(z * depth + lax.broadcasted_iota(jnp.int32, (1, depth), 1))
        batch = 16

        def split(g, _):
            at_row = pl.multiple_of(g * batch, batch)
            index = at_row + lax.broadcasted_iota(jnp.int32, (batch, 1), 0)
            chip = lax.div(index, 2 * step) * RINGS + xx
            owner = chip * 2 + lax.rem(lax.div(index, step), 2)
            column = owner * own + offsets[q] + lax.rem(index, step)
            keep = block_of(START + column) == row_block
            block = jnp.where(keep, gathered[pl.ds(pl.multiple_of(first + at_row, batch), batch), :], 0.0)
            hi = block.astype(jnp.bfloat16)
            lo = (block - hi.astype(jnp.float32)).astype(jnp.bfloat16)
            lhs[pl.ds(at_row, batch), 0:depth] = hi
            lhs[pl.ds(at_row, batch), depth:2 * depth] = hi
            lhs[pl.ds(at_row, batch), 2 * depth:3 * depth] = lo
            return 0

        lax.fori_loop(0, width // batch, split, 0)
        across = 256

        def product(m, _):
            lanes = pl.ds(pl.multiple_of(m * across, across), across)
            part[pl.ds(first, width), lanes] = jnp.dot(
                lhs[0:width, :], weights[:, lanes], preferred_element_type=jnp.float32
            )
            return 0

        lax.fori_loop(0, rows // across, product, 0)

    def add_up(q, dx, s):
        step = SIZES[q]
        chunk = 2 * step
        xx = shift(x, dx, RINGS)
        side = lax.div(xx, 2)
        odd = lax.rem(z + side, 2)
        near = lax.rem(lax.div(z - side + 9, 2), RINGS)
        first = group_first(q, dx)
        slot_first = offsets[q] * 2 * RINGS + (dx % RINGS) * chunk

        def rows_of(j, start, size):
            return pl.ds(pl.multiple_of(first + shift(near, j, RINGS) * chunk + start, 8), size)

        def wait_for(lane, slot_at, size):
            ref = brought.at[lane, slot_at, pl.ds(slot_first, size)]
            pltpu.make_async_copy(ref, ref, sum_sem.at[q, dx % RINGS, lane * 2 + slot_at]).wait()

        def send_on(lane, slot_at, src, size):
            pltpu.make_async_remote_copy(
                src_ref=part.at[src],
                dst_ref=brought.at[lane, slot_at, pl.ds(slot_first, size)],
                send_sem=sum_sent,
                recv_sem=sum_sem.at[q, dx % RINGS, lane * 2 + slot_at],
                device_id=along_z[1 - 2 * lane],
                device_id_type=MESH,
            ).start()

        @pl.when(odd == (s + 1) % 2)
        def _():
            if s == 5:
                for lane in range(2):
                    wait_for(lane, 1, chunk)
                where = pl.ds(slot_first, chunk)
                final = part[rows_of(0, 0, chunk), :] + brought[0, 1, where, :] + brought[1, 1, where, :]
                for i in range(2):
                    to = pl.multiple_of(lax.rem(xx, 2) * (2 * own) + i * own + offsets[q], 8)
                    o_ref[pl.ds(to, step), :] = final[i * step:(i + 1) * step, :]
                return
            for lane in range(2):
                start = lane * step
                j = {1: (2, 2), 2: (1, -2), 3: (1, -1), 4: (0, -1)}[s][lane]
                if s == 1:
                    send_on(lane, 0, rows_of(j, start, step), step)
                    continue
                if s == 2:
                    wait_for(lane, 0, step)
                    where = rows_of(j, start, step)
                    part[where, :] = part[where, :] + brought[lane, 0, pl.ds(slot_first, step), :]
                else:
                    wait_for(lane, s - 3, chunk)
                    where = rows_of(j, 0, chunk)
                    part[where, :] = part[where, :] + brought[lane, s - 3, pl.ds(slot_first, chunk), :]
                send_on(lane, 0 if s == 2 else 1, rows_of(j, 0, chunk), chunk)

    for op, q, a, b, c in ORDER:
        if op == 0:
            begin(q)
        elif op == 1:
            pass_on(q, a, b, c)
        elif op == 2:
            prepare()
        elif op == 3:
            multiply(q, a)
            add_up(q, a, 1)
        else:
            add_up(q, a, b)

    ref = gathered.at[pl.ds(0, (RINGS * RINGS - 1) * own)]
    pltpu.make_async_copy(ref, ref, gather_sent).wait()
    ref = gathered.at[pl.ds(0, RINGS * RINGS * own)]
    pltpu.make_async_copy(ref, ref, mate_sent).wait()
    ref = part.at[pl.ds(0, 28 * own)]
    pltpu.make_async_copy(ref, ref, sum_sent).wait()


def solution(mesh):
    devices, planes = mesh.shape["row"], mesh.shape["col"]
    phases = len(SIZES)

    def body(vectors, basis, block_units):
        rows, depth = vectors.shape
        own = basis.shape[1]
        f32, bf16 = jnp.float32, jnp.bfloat16
        dma = pltpu.SemaphoreType.DMA
        summed = pl.pallas_call(
            functools.partial(kernel, (rows, depth, own, planes)),
            out_shape=jax.ShapeDtypeStruct((own * devices // planes, rows), f32),
            in_specs=[
                pl.BlockSpec(memory_space=pltpu.SMEM),
                pl.BlockSpec(memory_space=pl.ANY),
                pl.BlockSpec(memory_space=pl.ANY),
            ],
            out_specs=pl.BlockSpec(memory_space=pltpu.VMEM),
            scratch_shapes=[
                pltpu.VMEM((own * devices, depth), f32),
                pltpu.VMEM((rows, depth), f32),
                pltpu.VMEM((3 * depth, rows), bf16),
                pltpu.VMEM((2 * RINGS * max(SIZES), 3 * depth), bf16),
                pltpu.VMEM((own * devices, rows), f32),
                pltpu.VMEM((2, 2, 2 * RINGS * own, rows), f32),
                dma,
                dma((phases,)),
                dma((phases, 2, RINGS * RINGS)),
                dma,
                dma((phases, RINGS)),
                dma,
                dma((phases, RINGS, 4)),
                dma,
            ],
            compiler_params=pltpu.CompilerParams(
                collective_id=0, has_side_effects=True, vmem_limit_bytes=63 * 1024 * 1024
            ),
            cost_estimate=pl.CostEstimate(
                flops=6 * rows * depth * own * devices, bytes_accessed=4 * rows * depth, transcendentals=0
            ),
        )(block_units, vectors, basis.T)
        return summed.T

    return jax.shard_map(
        body,
        mesh=mesh,
        in_specs=(P("row", "col"), P("col", "row"), P()),
        out_specs=P("row", "col"),
        check_vma=False,
    )
```
